32 devices in a mesh: grp: 4 (over x, core), tile: 8 (over z, y).
Axes of the slice: x: 2, y: 2, z: 4, core: 2. Of those that a mesh axis runs over, the one named last changes fastest.
Arguments:
- start_block: float32 [65536, 256], P(('grp', 'tile')), may hold values from -8 to 8
- dense_tiles: float32 [32, 2048, 2048], P(('grp', 'tile')), as said below
- basis: float32 [32, 48, 2048], P(('grp', 'tile')), may hold values from -0.125 to 0.125
- coupling: float32 [4, 8, 48, 1536], P(None, 'tile', None, 'grp'), as said below
- admissible: int32 [4, 8, 32], P(None, 'tile', 'grp'), may hold values from 0 to 1, as said below
Outputs:
- modes: float32 [65536, 256], P(('grp', 'tile'))
The draws below stay inside these ranges and needn't reach their ends.
Inputs may be any that keep to these rules, and one draw needn't show every extreme that they name: admissible is symmetric over tile pairs (the entry for row tile i and column tile j equals that for row tile j and column tile i) and 0 where the row tile equals the column tile. `dense_tiles`: each dense tile is symmetric: a positive scale times a diagonal plus an unstructured symmetric off-diagonal part. The coupling, read as a matrix of order 32 * 48, is symmetric: block S_ji is the transpose of S_ij.
All inputs are finite; a program needn't handle non-finite values.
Results may differ from the reference program's by a relative error of at most 0.0003.
Values sent between devices are 32-bit elements; how exact they have to be, the bound alone decides.
No kernel may reach another device: no remote copies, remote signals or barrier semaphores. Data moves between devices by JAX's collectives and lax.ppermute only.
A program may use at most 128 MiB of HBM per device.

```python
import jax
import jax.numpy as jnp
from jax import lax

TB = 2048
M = 256
K = 48
ITERS = 2
TILES = 32
N_GRP = 4
N_TILE = 8


def draw_start_block(key, part):
    shared_key = jax.random.fold_in(key, 41)
    own_key = jax.random.fold_in(key, 42)
    factor_key = jax.random.fold_in(key, 43)
    total_rows = TILES * TB
    shared = jnp.clip(jax.random.normal(shared_key, (total_rows, 1), jnp.float32), -6.0, 6.0)
    own = jnp.clip(jax.random.normal(own_key, (total_rows, M), jnp.float32), -6.0, 6.0)
    factors = jax.random.uniform(factor_key, (1, M), jnp.float32, 0.5, 1.2)
    weight = jnp.sqrt(jnp.float32(M) / jnp.float32(100000.0))
    return shared * factors + weight * own


def draw_dense_tiles(key, part):
    first = jax.random.fold_in(key, 11)
    second = jax.random.fold_in(key, 12)
    offdiag = jax.random.normal(first, (TILES, TB, TB), jnp.float32) / jnp.sqrt(jnp.float32(TB))
    offdiag = (offdiag + jnp.swapaxes(offdiag, 1, 2)) / jnp.sqrt(jnp.float32(2.0))
    leading = jax.random.uniform(second, (TILES, TB), jnp.float32, 3.0, 6.0)
    scales = 1.0 + 3.0 * jnp.arange(TILES, dtype=jnp.float32) / jnp.float32(max(TILES - 1, 1))
    ident = jnp.eye(TB, dtype=jnp.float32)
    return scales[:, None, None] * (offdiag + leading[:, :, None] * ident[None, :, :])


def draw_coupling(key, part):
    order = TILES * K
    whole = jax.random.normal(jax.random.fold_in(key, 31), (order, order), jnp.float32) / jnp.sqrt(jnp.float32(K))
    whole = (whole + whole.T) / jnp.sqrt(jnp.float32(2.0))
    return whole.reshape(N_GRP, N_TILE, K, order)


def draw_admissible(key, part):
    chosen = jax.random.randint(jax.random.fold_in(key, 21), (TILES, TILES), 0, 2)
    upper = jnp.triu(chosen, 1)
    both = upper + upper.T
    return both.reshape(N_GRP, N_TILE, TILES).astype(jnp.int32)


def steps_of(rng, dims, split, low, high):
    loudness, own = 1.0, jax.random.fold_in(rng, 6)
    for axis_at, shards_of in split:
        heights = jnp.exp(jax.random.uniform(jax.random.fold_in(own, axis_at), (shards_of,), jnp.float32, low / len(split), high / len(split)))
        loudness = loudness * jnp.repeat(heights, dims[axis_at] // shards_of).reshape([-1 if axis == axis_at else 1 for axis in range(len(dims))])
    return loudness


def normal_values(rng, shape, width, bound, cuts=(), kind=jnp.bfloat16):
    loudness = steps_of(rng, shape, cuts, -0.22, 0.18) if cuts else 1.0
    values = jax.random.normal(rng, shape, jnp.float32) * width * loudness
    return jnp.minimum(jnp.maximum(values, -bound), bound).astype(kind)


def setup_inputs(seed: int = 0) -> dict:
    key_list = jax.random.split(jax.random.key(seed), 6)
    start_block = draw_start_block(jax.random.fold_in(key_list[5], 71), 0)
    dense_tiles = draw_dense_tiles(jax.random.fold_in(key_list[5], 71), 0)
    basis = normal_values(key_list[2], (TILES, K, TB), TB ** -0.5, 0.125, ((0, 32),), jnp.float32)
    coupling = draw_coupling(jax.random.fold_in(key_list[5], 71), 0)
    admissible = draw_admissible(jax.random.fold_in(key_list[5], 71), 0)
    return dict(start_block=start_block, dense_tiles=dense_tiles, basis=basis, coupling=coupling, admissible=admissible)


def reference(start_block, dense_tiles, basis, coupling, admissible):
    hp = lax.Precision.HIGHEST
    flags = admissible.astype(jnp.float32)
    masked = coupling.reshape(N_GRP, N_TILE, K, TILES, K) * flags[:, :, None, :, None]
    masked = masked.reshape(TILES * K, TILES * K)

    def operate(field):
        pieces = field.reshape(TILES, TB, M)
        coeffs = jnp.einsum('tkr,trm->tkm', basis, pieces, precision=hp).reshape(TILES * K, M)
        summed = jnp.dot(masked, coeffs, precision=hp).reshape(TILES, K, M)
        far = jnp.einsum('tkr,tkm->trm', basis, summed, precision=hp)
        near = jnp.einsum('trs,tsm->trm', dense_tiles, pieces, precision=hp)
        return (far + near).reshape(TILES * TB, M)
    current = start_block
    for step in range(ITERS):
        image = operate(current)
        gram = jnp.dot(image.T, image, precision=hp) / jnp.float32(TILES * TB)
        lower = jnp.linalg.cholesky(gram)
        inverse = lax.linalg.triangular_solve(lower, jnp.eye(M, dtype=gram.dtype), left_side=True, lower=True)
        current = jnp.dot(image, inverse.T, precision=hp)
    return current
```

```python
import functools

import jax
import jax.numpy as jnp
from jax import lax
from jax.experimental import pallas as pl
from jax.experimental.pallas import tpu as pltpu
from jax.sharding import PartitionSpec as P


HP = lax.Precision.HIGHEST
SMEM = pl.BlockSpec(memory_space=pltpu.SMEM)
VMEM = pl.BlockSpec(memory_space=pltpu.VMEM)
VREG = (8, 128)


def down(x, row):
    return jnp.broadcast_to(x[row : row + 1, :], VREG)


def factor_inverse(t_ref, out_ref):
    n = t_ref.shape[0]
    halves = range(n // 128)
    lane = lax.broadcasted_iota(jnp.int32, VREG, 1)
    sub = lax.broadcasted_iota(jnp.int32, VREG, 0)
    for k in range(0, n, 8):
        h, at = k // 128, k % 128
        rows = [t_ref[k : k + 8, 128 * g : 128 * g + 128] for g in halves]
        cols = [jnp.broadcast_to(rows[h][:, at + c : at + c + 1], VREG) for c in range(8)]
        inside = (lane >= at) & (lane < at + 8)
        rows[h] = jnp.where(inside, jnp.where(lane - at == sub, 1.0, 0.0), rows[h])
        invs = jnp.zeros(VREG, jnp.float32)
        for j in range(8):
            inv = 1.0 / down(cols[j], j)
            invs = jnp.where(sub == j, inv, invs)
            if j == 7:
                break
            f = jnp.where(sub > j, cols[j] * inv, 0.0)
            for c in range(j + 1, 8):
                cols[c] = cols[c] - f * down(cols[c], j)
            for g in halves:
                rows[g] = rows[g] - f * down(rows[g], j)
        roots = jnp.sqrt(invs)
        for g in halves:
            if g > h:
                out = jnp.zeros(VREG, jnp.float32)
            else:
                out = rows[g] * roots
                if g == h:
                    out = jnp.where(lane < at + 8, out, 0.0)
            out_ref[k : k + 8, 128 * g : 128 * g + 128] = out
        if k + 8 == n:
            break
        rows = [x * invs for x in rows]
        for c in range(7, 0, -1):
            f = jnp.where(sub < c, cols[c] * invs, 0.0)
            for g in halves:
                rows[g] = rows[g] - f * down(rows[g], c)
        wide = [[down(rows[g], i) for i in range(8)] for g in halves]
        for r in range(k + 8, n, 8):
            now = [t_ref[r : r + 8, 128 * g : 128 * g + 128] for g in halves]
            f = [jnp.broadcast_to(now[h][:, at + i : at + i + 1], VREG) for i in range(8)]
            now[h] = jnp.where(inside, 0.0, now[h])
            for g in halves:
                w = wide[g]
                low = (f[0] * w[0] + f[1] * w[1]) + (f[2] * w[2] + f[3] * w[3])
                high = (f[4] * w[4] + f[5] * w[5]) + (f[6] * w[6] + f[7] * w[7])
                t_ref[r : r + 8, 128 * g : 128 * g + 128] = now[g] - (low + high)


def triangle_masks(m):
    row = lax.broadcasted_iota(jnp.int32, (m, m), 0)
    col = lax.broadcasted_iota(jnp.int32, (m, m), 1)
    return row, col


def pack_kernel(side_ref, gram_ref, mine_ref, theirs_ref):
    m = gram_ref.shape[0] // 2
    row, col = triangle_masks(m)
    second = gram_ref[m:, m:]
    cross = gram_ref[m:, :m]
    both = jnp.where(row >= col, gram_ref[:m, :m], second)
    diag = jnp.sum(jnp.where(row == col, second, 0.0), axis=0, keepdims=True)
    south = side_ref[0] == 0
    mine_ref[:m] = jnp.where(south, cross, both)
    theirs_ref[:m] = jnp.where(south, both, cross)
    mine_ref[m:] = jnp.broadcast_to(diag, (8, m))
    theirs_ref[m:] = jnp.broadcast_to(diag, (8, m))


def pack(side, gram):
    m = gram.shape[0] // 2
    part = jax.ShapeDtypeStruct((m + 8, m), jnp.float32)
    return pl.pallas_call(
        pack_kernel, out_shape=(part, part), in_specs=[SMEM, VMEM], out_specs=(VMEM, VMEM), name="pack",
        cost_estimate=pl.CostEstimate(flops=8 * m * m * 40, bytes_accessed=16 * m * m, transcendentals=0),
    )(side, gram)


def factor_kernel(scale, side_ref, mine_ref, theirs_ref, out_ref, t_ref):
    m = mine_ref.shape[1]
    row, col = triangle_masks(m)
    south = side_ref[0] == 0
    cross = jnp.where(south, mine_ref[:m], theirs_ref[:m]) * scale
    both = jnp.where(south, theirs_ref[:m], mine_ref[:m]) * scale
    diag = jnp.where(south, theirs_ref[m : m + 1], mine_ref[m : m + 1]) * scale
    flip = both.T
    t_ref[:m, :m] = jnp.where(row >= col, both, flip)
    t_ref[m:, m:] = jnp.where(row == col, jnp.broadcast_to(diag, (m, m)), jnp.where(row < col, both, flip))
    t_ref[m:, :m] = cross
    t_ref[:m, m:] = cross.T
    factor_inverse(t_ref, out_ref)


def factor(side, mine, theirs, scale):
    m = mine.shape[1]
    return pl.pallas_call(
        functools.partial(factor_kernel, scale),
        out_shape=jax.ShapeDtypeStruct((2 * m, 2 * m), jnp.float32),
        in_specs=[SMEM, VMEM, VMEM], out_specs=VMEM, scratch_shapes=[pltpu.VMEM((2 * m, 2 * m), jnp.float32)],
        name="factor",
        cost_estimate=pl.CostEstimate(flops=40_000_000, bytes_accessed=32 * m * m, transcendentals=0),
    )(side, mine, theirs)


def couple_kernel(order, place_ref, masked_ref, *refs):
    blocks, far_ref, near_ref, held = refs[: len(order)], refs[-3], refs[-2], refs[-1]
    tile, group = place_ref[0], place_ref[1]
    width = blocks[0].shape[0] // len(order[0])
    for names, block in zip(order, blocks):
        for at, name in enumerate(names):
            start = pl.multiple_of((tile ^ name) * width, 8)
            held[pl.ds(start, width), :] = block[at * width : (at + 1) * width, :]
    total = jnp.dot(masked_ref[...], held[...], precision=HP, preferred_element_type=jnp.float32)
    held[: total.shape[0], :] = total
    groups = total.shape[0] // width
    count = groups // 2
    for at in range(count):
        near_ref[at * width : (at + 1) * width] = held[pl.ds(pl.multiple_of((group ^ at) * width, 8), width), :]
        far_ref[at * width : (at + 1) * width] = held[pl.ds(pl.multiple_of((group ^ (at + count)) * width, 8), width), :]


def couple(place, masked, blocks, order, width):
    rows, depth = masked.shape
    modes = blocks[0].shape[1]
    half = jax.ShapeDtypeStruct((rows // 2, modes), jnp.float32)
    return pl.pallas_call(
        functools.partial(couple_kernel, order),
        out_shape=(half, half), in_specs=[SMEM, VMEM] + [VMEM] * len(blocks), out_specs=(VMEM, VMEM),
        scratch_shapes=[pltpu.VMEM((max(rows, depth), modes), jnp.float32)], name="couple",
        cost_estimate=pl.CostEstimate(flops=12 * rows * depth * modes, bytes_accessed=4 * rows * depth, transcendentals=0),
    )(place, masked, *blocks)


def swap(x, axis, bit):
    return lax.ppermute(x, axis, [(i, i ^ bit) for i in range(lax.axis_size(axis))])


def body(start_block, dense_tiles, basis, coupling, admissible):
    groups = coupling.shape[0]
    width = basis.shape[1]
    span = coupling.shape[3] // width
    tiles = lax.axis_size("tile")
    total_rows = lax.axis_size("grp") * tiles * start_block.shape[0]
    flags = admissible.astype(jnp.float32).reshape(groups, 1, span, 1)
    masked = (coupling.reshape(groups, width, span, width) * flags).reshape(groups * width, span * width)
    dense = dense_tiles[0]
    rows_basis = basis[0]
    group, tile = lax.axis_index("grp"), lax.axis_index("tile")
    place = jnp.stack([tile, group]).astype(jnp.int32)
    side = jnp.stack([group % 2]).astype(jnp.int32)

    def couple_all(coeffs):
        blocks, order, held, names = [coeffs], [(0,)], coeffs, (0,)
        bit = tiles // 2
        while bit:
            got = swap(held, "tile", bit)
            blocks.append(got)
            order.append(tuple(name ^ bit for name in names))
            names = names + order[-1]
            bit //= 2
            if bit:
                held = jnp.concatenate([held, got])
        far, near = couple(place, masked, blocks, tuple(order), width)
        bit = groups // 2
        while True:
            near = near + swap(far, "grp", bit)
            bit //= 2
            if not bit:
                return near
            far, near = near[near.shape[0] // 2 :], near[: near.shape[0] // 2]

    def whitening(field):
        gram = lax.dot_general(field, field, (((0,), (0,)), ((), ())), precision=HP)
        mine, theirs = pack(side, gram)
        mine = mine + swap(theirs, "grp", 1)
        bit = groups // 2
        while bit > 1:
            mine = mine + swap(mine, "grp", bit)
            bit //= 2
        bit = 1
        while bit < tiles:
            mine = mine + swap(mine, "tile", bit)
            bit *= 2
        theirs = swap(mine, "grp", 1)
        return factor(side, mine, theirs, 1.0 / total_rows)

    def near_of(field):
        return jnp.dot(dense, field, precision=NEAR)

    def far_of(summed):
        return lax.dot_general(rows_basis, summed, (((0,), (0,)), ((), ())), precision=HP)

    def whiten(field, inverse):
        return lax.dot_general(field, inverse, (((1,), (1,)), ((), ())), precision=HP)

    image = near_of(start_block) + far_of(couple_all(jnp.dot(rows_basis, start_block, precision=HP)))
    inverse = whitening(image)
    further = near_of(image) + far_of(couple_all(jnp.dot(rows_basis, image, precision=HP)))
    image = whiten(further, inverse)
    inverse = whitening(image)
    return whiten(image, inverse)


NEAR = HP


def solution(mesh):
    placed = (
        P(("grp", "tile"), None),
        P(("grp", "tile"), None, None),
        P(("grp", "tile"), None, None),
        P(None, "tile", None, "grp"),
        P(None, "tile", "grp"),
    )
    return jax.shard_map(
        body, mesh=mesh, in_specs=placed, out_specs=P(("grp", "tile"), None), check_vma=False
    )
```

```python
import functools

import jax
import jax.numpy as jnp
from jax import lax
from jax.experimental import pallas as pl
from jax.experimental.pallas import tpu as pltpu
from jax.sharding import PartitionSpec as P


HP = lax.Precision.HIGHEST
SMEM = pl.BlockSpec(memory_space=pltpu.SMEM)
VMEM = pl.BlockSpec(memory_space=pltpu.VMEM)
VREG = (8, 128)


def down(x, row):
    return jnp.broadcast_to(x[row : row + 1, :], VREG)


def factor_inverse(t_ref, out_ref):
    n = t_ref.shape[0]
    halves = range(n // 128)
    lane = lax.broadcasted_iota(jnp.int32, VREG, 1)
    sub = lax.broadcasted_iota(jnp.int32, VREG, 0)
    every = sub < 8
    rows = [t_ref[:8, 128 * g : 128 * g + 128] for g in halves]
    for k in range(0, n, 8):
        h, at = k // 128, k % 128
        cols = [jnp.where(every, jnp.broadcast_to(rows[h][:, at + c : at + c + 1], VREG), 0.0) for c in range(8)]
        inside = (lane >= at) & (lane < at + 8)
        rows[h] = jnp.where(inside, jnp.where(lane - at == sub, 1.0, 0.0), rows[h])
        pivots = jnp.ones(VREG, jnp.float32)
        done = list(rows)
        for j in range(8):
            pivot = down(cols[j], j)
            pivots = jnp.where(sub == j, pivot, pivots)
            f = jnp.where(sub == j, 0.0, cols[j])
            for c in range(j + 1, 8):
                cols[c] = cols[c] - (f * down(cols[c], j)) / pivot
            for g in halves:
                done[g] = jnp.where(sub == j, rows[g], done[g])
                rows[g] = rows[g] - (f * down(rows[g], j)) / pivot
        roots = lax.rsqrt(pivots)
        for g in halves:
            if g > h:
                out = jnp.zeros(VREG, jnp.float32)
            else:
                out = done[g] * roots
                if g == h:
                    out = jnp.where(lane < at + 8, out, 0.0)
            out_ref[k : k + 8, 128 * g : 128 * g + 128] = out
        if k + 8 == n:
            break
        rows = [x / pivots for x in rows]
        wide = [[down(rows[g], i) for i in range(8)] for g in halves]
        for r in range(k + 8, n, 8):
            now = [t_ref[r : r + 8, 128 * g : 128 * g + 128] for g in halves]
            f = [jnp.broadcast_to(now[h][:, at + i : at + i + 1], VREG) for i in range(8)]
            now[h] = jnp.where(inside, 0.0, now[h])
            for g in halves:
                w = wide[g]
                low = (f[0] * w[0] + f[1] * w[1]) + (f[2] * w[2] + f[3] * w[3])
                high = (f[4] * w[4] + f[5] * w[5]) + (f[6] * w[6] + f[7] * w[7])
                now[g] = now[g] - (low + high)
            if r == k + 8:
                rows = now
            else:
                for g in halves:
                    t_ref[r : r + 8, 128 * g : 128 * g + 128] = now[g]


def split(x, parts):
    terms = []
    for at in range(parts):
        terms.append(x.astype(jnp.bfloat16))
        if at + 1 < parts:
            x = x - terms[-1].astype(jnp.float32)
    return terms


def mul(a, b, contract=(1, 0)):
    return lax.dot_general(a, b, (((contract[0],), (contract[1],)), ((), ())), preferred_element_type=jnp.float32)


def triangle_masks(m):
    row = lax.broadcasted_iota(jnp.int32, (m, m), 0)
    col = lax.broadcasted_iota(jnp.int32, (m, m), 1)
    return row, col


def pack_into(side_ref, gram, mine_ref, theirs_ref):
    m = gram.shape[0] // 2
    row, col = triangle_masks(m)
    second = gram[m:, m:]
    cross = gram[m:, :m]
    both = jnp.where(row >= col, gram[:m, :m], second)
    diag = jnp.sum(jnp.where(row == col, second, 0.0), axis=0, keepdims=True)
    south = side_ref[0] == 0
    mine_ref[:m] = jnp.where(south, cross, both)
    theirs_ref[:m] = jnp.where(south, both, cross)
    mine_ref[m:] = jnp.broadcast_to(diag, (8, m))
    theirs_ref[m:] = jnp.broadcast_to(diag, (8, m))


def unpack_into(scale, side_ref, mine_ref, theirs_ref, t_ref):
    m = mine_ref.shape[1]
    row, col = triangle_masks(m)
    south = side_ref[0] == 0
    cross = jnp.where(south, mine_ref[:m], theirs_ref[:m]) * scale
    both = jnp.where(south, theirs_ref[:m], mine_ref[:m]) * scale
    diag = jnp.where(south, theirs_ref[m : m + 1], mine_ref[m : m + 1]) * scale
    flip = both.T
    t_ref[:m, :m] = jnp.where(row >= col, both, flip)
    t_ref[m:, m:] = jnp.where(row == col, jnp.broadcast_to(diag, (m, m)), jnp.where(row < col, both, flip))
    t_ref[m:, :m] = cross
    t_ref[:m, m:] = cross.T


def stack_basis(basis_ref, stacked):
    width = basis_ref.shape[0]
    high, low = split(basis_ref[...], 2)
    for at, part in enumerate((high, low, high, high, low)):
        stacked[at * width : (at + 1) * width] = part


def stack_sums(summed_ref):
    high, mid, low = split(summed_ref[...], 3)
    return jnp.concatenate([high, high, mid, low, mid], axis=0)


def gram_terms(field, total, cross):
    high, mid = split(field, 2)
    total[...] += mul(high, high, (0, 0)) + mul(mid, mid, (0, 0))
    cross[...] += mul(high, mid, (0, 0))


CHUNK = 1024


def chunks(rows, step):
    def run(at, carry):
        step(pl.ds(pl.multiple_of(at * CHUNK, CHUNK), CHUNK))
        return carry

    lax.fori_loop(0, rows // CHUNK, run, 0)


def mix_kernel(side_ref, near_ref, basis_ref, summed_ref, image_ref, coeffs_ref, mine_ref, theirs_ref,
               stacked, total, cross, parts):
    width = basis_ref.shape[0]
    stack_basis(basis_ref, stacked)
    sums = stack_sums(summed_ref)
    total[...] = jnp.zeros_like(total)
    cross[...] = jnp.zeros_like(cross)
    parts[...] = jnp.zeros_like(parts)

    def step(rows):
        image = near_ref[rows, :] + mul(stacked[:, rows], sums, (0, 0))
        image_ref[rows, :] = image
        high, mid, low = split(image, 3)
        total[...] += mul(high, high, (0, 0)) + mul(mid, mid, (0, 0))
        cross[...] += mul(high, mid, (0, 0))
        two = stacked[: 2 * width, rows]
        both = mul(two, high) + mul(two, mid)
        parts[...] += both[:width] + both[width:] + mul(two[:width], low)

    chunks(near_ref.shape[0], step)
    coeffs_ref[...] = parts[...]
    pack_into(side_ref, total[...] + (cross[...] + cross[...].T), mine_ref, theirs_ref)


def mix(side, near, basis, summed):
    rows, modes = near.shape
    width = basis.shape[0]
    part = jax.ShapeDtypeStruct((modes // 2 + 8, modes // 2), jnp.float32)
    square = pltpu.VMEM((modes, modes), jnp.float32)
    return pl.pallas_call(
        mix_kernel,
        out_shape=(jax.ShapeDtypeStruct((rows, modes), jnp.float32), jax.ShapeDtypeStruct((width, modes), jnp.float32), part, part),
        in_specs=[SMEM, VMEM, VMEM, VMEM], out_specs=(VMEM,) * 4,
        scratch_shapes=[pltpu.VMEM((5 * width, rows), jnp.bfloat16), square, square, pltpu.VMEM((width, modes), jnp.float32)],
        name="mix", cost_estimate=pl.CostEstimate(flops=12 * rows * modes * modes, bytes_accessed=8 * rows * modes, transcendentals=0),
    )(side, near, basis, summed)


def middle_kernel(scale, side_ref, mine_ref, theirs_ref, near_ref, basis_ref, summed_ref, image_ref, out_mine_ref, out_theirs_ref,
                  t_ref, inverse, stacked, total, cross):
    unpack_into(scale, side_ref, mine_ref, theirs_ref, t_ref)
    factor_inverse(t_ref, inverse)
    stack_basis(basis_ref, stacked)
    sums = stack_sums(summed_ref)
    total[...] = jnp.zeros_like(total)
    cross[...] = jnp.zeros_like(cross)
    first, second = split(inverse[...], 2)

    def step(rows):
        further = near_ref[rows, :] + mul(stacked[:, rows], sums, (0, 0))
        high, mid, low = split(further, 3)
        image = (mul(high, first, (1, 1)) + mul(mid, first, (1, 1))) + (mul(high, second, (1, 1)) + (mul(mid, second, (1, 1)) + mul(low, first, (1, 1))))
        image_ref[rows, :] = image
        gram_terms(image, total, cross)

    chunks(near_ref.shape[0], step)
    pack_into(side_ref, total[...] + (cross[...] + cross[...].T), out_mine_ref, out_theirs_ref)


def middle(side, mine, theirs, scale, near, basis, summed):
    rows, modes = near.shape
    width = basis.shape[0]
    part = jax.ShapeDtypeStruct(mine.shape, jnp.float32)
    square = pltpu.VMEM((modes, modes), jnp.float32)
    return pl.pallas_call(
        functools.partial(middle_kernel, scale),
        out_shape=(jax.ShapeDtypeStruct((rows, modes), jnp.float32), part, part),
        in_specs=[SMEM] + [VMEM] * 5, out_specs=(VMEM,) * 3,
        scratch_shapes=[square, square, pltpu.VMEM((5 * width, rows), jnp.bfloat16), square, square],
        name="middle", cost_estimate=pl.CostEstimate(flops=40_000_000, bytes_accessed=8 * rows * modes, transcendentals=0),
    )(side, mine, theirs, near, basis, summed)


def last_kernel(scale, side_ref, mine_ref, theirs_ref, image_ref, out_ref, t_ref, inverse):
    unpack_into(scale, side_ref, mine_ref, theirs_ref, t_ref)
    factor_inverse(t_ref, inverse)
    first, second = split(inverse[...], 2)

    def step(rows):
        high, mid = split(image_ref[rows, :], 2)
        out_ref[rows, :] = mul(high, first, (1, 1)) + (mul(mid, first, (1, 1)) + (mul(high, second, (1, 1)) + mul(mid, second, (1, 1))))

    chunks(image_ref.shape[0], step)


def last(side, mine, theirs, scale, image):
    modes = image.shape[1]
    square = pltpu.VMEM((modes, modes), jnp.float32)
    return pl.pallas_call(
        functools.partial(last_kernel, scale),
        out_shape=jax.ShapeDtypeStruct(image.shape, jnp.float32),
        in_specs=[SMEM] + [VMEM] * 3, out_specs=VMEM, scratch_shapes=[square, square],
        name="last", cost_estimate=pl.CostEstimate(flops=40_000_000, bytes_accessed=8 * image.size, transcendentals=0),
    )(side, mine, theirs, image)


def near_kernel(dense_ref, field_ref, out_ref, high, mid, low):
    @pl.when(pl.program_id(0) == 0)
    def _():
        high[...], mid[...], low[...] = split(field_ref[...], 3)

    top, rest = split(dense_ref[...], 2)
    out_ref[...] = mul(top, high[...]) + (mul(top, mid[...]) + (mul(rest, high[...]) + (mul(rest, mid[...]) + mul(top, low[...]))))


BLOCK = 512


def near_of(dense, field):
    rows, depth = dense.shape
    modes = field.shape[1]
    term = pltpu.VMEM(field.shape, jnp.bfloat16)
    return pl.pallas_call(
        near_kernel, grid=(rows // BLOCK,),
        out_shape=jax.ShapeDtypeStruct((rows, modes), jnp.float32),
        in_specs=[pl.BlockSpec((BLOCK, depth), lambda i: (i, 0)), pl.BlockSpec((depth, modes), lambda i: (0, 0))],
        out_specs=pl.BlockSpec((BLOCK, modes), lambda i: (i, 0)), scratch_shapes=[term, term, term],
        name="near", cost_estimate=pl.CostEstimate(flops=10 * rows * depth * modes, bytes_accessed=4 * rows * depth, transcendentals=0),
    )(dense, field)


def couple_kernel(order, place_ref, masked_ref, *refs):
    blocks, far_ref, near_ref, held = refs[: len(order)], refs[-3], refs[-2], refs[-1]
    tile, group = place_ref[0], place_ref[1]
    width = blocks[0].shape[0] // len(order[0])
    for names, block in zip(order, blocks):
        for at, name in enumerate(names):
            start = pl.multiple_of((tile ^ name) * width, 8)
            held[pl.ds(start, width), :] = block[at * width : (at + 1) * width, :]
    total = jnp.dot(masked_ref[...], held[...], precision=HP, preferred_element_type=jnp.float32)
    held[: total.shape[0], :] = total
    groups = total.shape[0] // width
    count = groups // 2
    for at in range(count):
        near_ref[at * width : (at + 1) * width] = held[pl.ds(pl.multiple_of((group ^ at) * width, 8), width), :]
        far_ref[at * width : (at + 1) * width] = held[pl.ds(pl.multiple_of((group ^ (at + count)) * width, 8), width), :]


def couple(place, masked, blocks, order, width):
    rows, depth = masked.shape
    modes = blocks[0].shape[1]
    half = jax.ShapeDtypeStruct((rows // 2, modes), jnp.float32)
    return pl.pallas_call(
        functools.partial(couple_kernel, order),
        out_shape=(half, half), in_specs=[SMEM, VMEM] + [VMEM] * len(blocks), out_specs=(VMEM, VMEM),
        scratch_shapes=[pltpu.VMEM((max(rows, depth), modes), jnp.float32)], name="couple",
        cost_estimate=pl.CostEstimate(flops=12 * rows * depth * modes, bytes_accessed=4 * rows * depth, transcendentals=0),
    )(place, masked, *blocks)


def swap(x, axis, bit):
    return lax.ppermute(x, axis, [(i, i ^ bit) for i in range(lax.axis_size(axis))])


def body(start_block, dense_tiles, basis, coupling, admissible):
    groups = coupling.shape[0]
    width = basis.shape[1]
    span = coupling.shape[3] // width
    tiles = lax.axis_size("tile")
    total_rows = lax.axis_size("grp") * tiles * start_block.shape[0]
    flags = admissible.astype(jnp.float32).reshape(groups, 1, span, 1)
    masked = (coupling.reshape(groups, width, span, width) * flags).reshape(groups * width, span * width)
    dense = dense_tiles[0]
    rows_basis = basis[0]
    group, tile = lax.axis_index("grp"), lax.axis_index("tile")
    place = jnp.stack([tile, group]).astype(jnp.int32)
    side = jnp.stack([group % 2]).astype(jnp.int32)

    def couple_all(coeffs):
        blocks, order, held, names = [coeffs], [(0,)], coeffs, (0,)
        bit = tiles // 2
        while bit:
            got = swap(held, "tile", bit)
            blocks.append(got)
            order.append(tuple(name ^ bit for name in names))
            names = names + order[-1]
            bit //= 2
            if bit:
                held = jnp.concatenate([held, got])
        far, near = couple(place, masked, blocks, tuple(order), width)
        bit = groups // 2
        while True:
            near = near + swap(far, "grp", bit)
            bit //= 2
            if not bit:
                return near
            far, near = near[near.shape[0] // 2 :], near[: near.shape[0] // 2]

    scale = 1.0 / total_rows

    def add_devices(mine, theirs):
        mine = mine + swap(theirs, "grp", 1)
        bit = groups // 2
        while bit > 1:
            mine = mine + swap(mine, "grp", bit)
            bit //= 2
        bit = 1
        while bit < tiles:
            mine = mine + swap(mine, "tile", bit)
            bit *= 2
        return mine, swap(mine, "grp", 1)

    summed = couple_all(jnp.dot(rows_basis, start_block, precision=HP))
    image, coeffs, mine, theirs = mix(side, near_of(dense, start_block), rows_basis, summed)
    mine, theirs = add_devices(mine, theirs)
    summed = couple_all(coeffs)
    image, mine, theirs = middle(side, mine, theirs, scale, near_of(dense, image), rows_basis, summed)
    mine, theirs = add_devices(mine, theirs)
    return last(side, mine, theirs, scale, image)


def solution(mesh):
    placed = (
        P(("grp", "tile"), None),
        P(("grp", "tile"), None, None),
        P(("grp", "tile"), None, None),
        P(None, "tile", None, "grp"),
        P(None, "tile", "grp"),
    )
    return jax.shard_map(
        body, mesh=mesh, in_specs=placed, out_specs=P(("grp", "tile"), None), check_vma=False
    )
```

```python
import functools

import jax
import jax.numpy as jnp
from jax import lax
from jax.experimental import pallas as pl
from jax.experimental.pallas import tpu as pltpu
from jax.sharding import PartitionSpec as P


HP = lax.Precision.HIGHEST
SMEM = pl.BlockSpec(memory_space=pltpu.SMEM)
VMEM = pl.BlockSpec(memory_space=pltpu.VMEM)
VREG = (8, 128)


def down(x, row):
    return jnp.broadcast_to(x[row : row + 1, :], VREG)


def factor_inverse(t_ref, out_ref):
    n = t_ref.shape[0]
    halves = range(n // 128)
    lane = lax.broadcasted_iota(jnp.int32, VREG, 1)
    sub = lax.broadcasted_iota(jnp.int32, VREG, 0)
    every = sub < 8
    rows = [t_ref[:8, 128 * g : 128 * g + 128] for g in halves]
    for k in range(0, n, 8):
        h, at = k // 128, k % 128
        cols = [jnp.where(every, jnp.broadcast_to(rows[h][:, at + c : at + c + 1], VREG), 0.0) for c in range(8)]
        inside = (lane >= at) & (lane < at + 8)
        rows[h] = jnp.where(inside, jnp.where(lane - at == sub, 1.0, 0.0), rows[h])
        pivots = jnp.ones(VREG, jnp.float32)
        done = list(rows)
        for j in range(8):
            pivot = down(cols[j], j)
            pivots = jnp.where(sub == j, pivot, pivots)
            f = jnp.where(sub == j, 0.0, cols[j])
            for c in range(j + 1, 8):
                cols[c] = cols[c] - (f * down(cols[c], j)) / pivot
            for g in halves:
                done[g] = jnp.where(sub == j, rows[g], done[g])
                rows[g] = rows[g] - (f * down(rows[g], j)) / pivot
        roots = lax.rsqrt(pivots)
        for g in halves:
            if g > h:
                out = jnp.zeros(VREG, jnp.float32)
            else:
                out = done[g] * roots
                if g == h:
                    out = jnp.where(lane < at + 8, out, 0.0)
            out_ref[k : k + 8, 128 * g : 128 * g + 128] = out
        if k + 8 == n:
            break
        rows = [x / pivots for x in rows]
        wide = [[down(rows[g], i) for i in range(8)] for g in halves]
        for r in range(k + 8, n, 8):
            now = [t_ref[r : r + 8, 128 * g : 128 * g + 128] for g in halves]
            f = [jnp.broadcast_to(now[h][:, at + i : at + i + 1], VREG) for i in range(8)]
            now[h] = jnp.where(inside, 0.0, now[h])
            for g in halves:
                w = wide[g]
                low = (f[0] * w[0] + f[1] * w[1]) + (f[2] * w[2] + f[3] * w[3])
                high = (f[4] * w[4] + f[5] * w[5]) + (f[6] * w[6] + f[7] * w[7])
                now[g] = now[g] - (low + high)
            if r == k + 8:
                rows = now
            else:
                for g in halves:
                    t_ref[r : r + 8, 128 * g : 128 * g + 128] = now[g]


def split(x, parts):
    terms = []
    for at in range(parts):
        terms.append(x.astype(jnp.bfloat16))
        if at + 1 < parts:
            x = x - terms[-1].astype(jnp.float32)
    return terms


def mul(a, b, contract=(1, 0)):
    return lax.dot_general(a, b, (((contract[0],), (contract[1],)), ((), ())), preferred_element_type=jnp.float32)


def triangle_masks(m):
    row = lax.broadcasted_iota(jnp.int32, (m, m), 0)
    col = lax.broadcasted_iota(jnp.int32, (m, m), 1)
    return row, col


def pack_into(side_ref, gram, mine_ref, theirs_ref):
    m = gram.shape[0] // 2
    row, col = triangle_masks(m)
    second = gram[m:, m:]
    cross = gram[m:, :m]
    both = jnp.where(row >= col, gram[:m, :m], second)
    diag = jnp.sum(jnp.where(row == col, second, 0.0), axis=0, keepdims=True)
    south = side_ref[0] == 0
    mine_ref[:m] = jnp.where(south, cross, both)
    theirs_ref[:m] = jnp.where(south, both, cross)
    mine_ref[m:] = jnp.broadcast_to(diag, (8, m))
    theirs_ref[m:] = jnp.broadcast_to(diag, (8, m))


def unpack_into(scale, side_ref, mine_ref, theirs_ref, t_ref):
    m = mine_ref.shape[1]
    row, col = triangle_masks(m)
    south = side_ref[0] == 0
    cross = jnp.where(south, mine_ref[:m], theirs_ref[:m]) * scale
    both = jnp.where(south, theirs_ref[:m], mine_ref[:m]) * scale
    diag = jnp.where(south, theirs_ref[m : m + 1], mine_ref[m : m + 1]) * scale
    flip = both.T
    t_ref[:m, :m] = jnp.where(row >= col, both, flip)
    t_ref[m:, m:] = jnp.where(row == col, jnp.broadcast_to(diag, (m, m)), jnp.where(row < col, both, flip))
    t_ref[m:, :m] = cross
    t_ref[:m, m:] = cross.T


def stack_basis(basis_ref, stacked):
    width = basis_ref.shape[0]
    high, low = split(basis_ref[...], 2)
    for at, part in enumerate((high, low, high, high, low)):
        stacked[at * width : (at + 1) * width] = part


def stack_sums(summed_ref):
    high, mid, low = split(summed_ref[...], 3)
    return jnp.concatenate([high, high, mid, low, mid], axis=0)


def gram_terms(field, total, cross):
    high, mid = split(field, 2)
    total[...] += mul(high, high, (0, 0)) + mul(mid, mid, (0, 0))
    cross[...] += mul(high, mid, (0, 0))


CHUNK = 512


def chunks(rows, step):
    def run(at, carry):
        step(pl.ds(pl.multiple_of(at * CHUNK, CHUNK), CHUNK))
        return carry

    lax.fori_loop(0, rows // CHUNK, run, 0)


def piece_rows(pieces, step):
    start = 0
    for piece in pieces:
        step(pl.ds(start, piece.shape[0]), piece)
        start += piece.shape[0]


def mix_kernel(side_ref, basis_ref, summed_ref, *refs):
    pieces, (image_ref, coeffs_ref, mine_ref, theirs_ref, stacked, total, cross, parts) = refs[:-8], refs[-8:]
    width = basis_ref.shape[0]
    stack_basis(basis_ref, stacked)
    sums = stack_sums(summed_ref)
    total[...] = jnp.zeros_like(total)
    cross[...] = jnp.zeros_like(cross)
    parts[...] = jnp.zeros_like(parts)

    def step(rows, piece):
        image = piece[...] + mul(stacked[:, rows], sums, (0, 0))
        image_ref[rows, :] = image
        high, mid, low = split(image, 3)
        total[...] += mul(high, high, (0, 0)) + mul(mid, mid, (0, 0))
        cross[...] += mul(high, mid, (0, 0))
        two = stacked[: 2 * width, rows]
        both = mul(two, high) + mul(two, mid)
        parts[...] += both[:width] + both[width:] + mul(two[:width], low)

    piece_rows(pieces, step)
    coeffs_ref[...] = parts[...]
    pack_into(side_ref, total[...] + (cross[...] + cross[...].T), mine_ref, theirs_ref)


def mix(side, pieces, basis, summed):
    rows, modes = basis.shape[1], summed.shape[1]
    width = basis.shape[0]
    part = jax.ShapeDtypeStruct((modes // 2 + 8, modes // 2), jnp.float32)
    square = pltpu.VMEM((modes, modes), jnp.float32)
    return pl.pallas_call(
        mix_kernel,
        out_shape=(jax.ShapeDtypeStruct((rows, modes), jnp.float32), jax.ShapeDtypeStruct((width, modes), jnp.float32), part, part),
        in_specs=[SMEM, VMEM, VMEM] + [VMEM] * len(pieces), out_specs=(VMEM,) * 4,
        scratch_shapes=[pltpu.VMEM((5 * width, rows), jnp.bfloat16), square, square, pltpu.VMEM((width, modes), jnp.float32)],
        name="mix", compiler_params=pltpu.CompilerParams(vmem_limit_bytes=24 * 2**20), cost_estimate=pl.CostEstimate(flops=12 * rows * modes * modes, bytes_accessed=8 * rows * modes, transcendentals=0),
    )(side, basis, summed, *pieces)


def factor_kernel(scale, side_ref, mine_ref, theirs_ref, out_ref, t_ref):
    unpack_into(scale, side_ref, mine_ref, theirs_ref, t_ref)
    factor_inverse(t_ref, out_ref)


def factor(side, mine, theirs, scale):
    modes = 2 * mine.shape[1]
    return pl.pallas_call(
        functools.partial(factor_kernel, scale),
        out_shape=jax.ShapeDtypeStruct((modes, modes), jnp.float32),
        in_specs=[SMEM, VMEM, VMEM], out_specs=VMEM, scratch_shapes=[pltpu.VMEM((modes, modes), jnp.float32)],
        name="factor", compiler_params=pltpu.CompilerParams(vmem_limit_bytes=16 * 2**20),
        cost_estimate=pl.CostEstimate(flops=40_000_000, bytes_accessed=8 * modes * modes, transcendentals=0),
    )(side, mine, theirs)


def middle_kernel(side_ref, inverse, basis_ref, summed_ref, *refs):
    pieces, (image_ref, out_mine_ref, out_theirs_ref, stacked, total, cross) = refs[:-6], refs[-6:]
    stack_basis(basis_ref, stacked)
    sums = stack_sums(summed_ref)
    total[...] = jnp.zeros_like(total)
    cross[...] = jnp.zeros_like(cross)
    first, second = split(inverse[...], 2)

    def step(rows, piece):
        further = piece[...] + mul(stacked[:, rows], sums, (0, 0))
        high, mid, low = split(further, 3)
        image = (mul(high, first, (1, 1)) + mul(mid, first, (1, 1))) + (mul(high, second, (1, 1)) + (mul(mid, second, (1, 1)) + mul(low, first, (1, 1))))
        image_ref[rows, :] = image
        gram_terms(image, total, cross)

    piece_rows(pieces, step)
    pack_into(side_ref, total[...] + (cross[...] + cross[...].T), out_mine_ref, out_theirs_ref)


def middle(side, inverse, pieces, basis, summed):
    rows, modes = basis.shape[1], summed.shape[1]
    width = basis.shape[0]
    part = jax.ShapeDtypeStruct((modes // 2 + 8, modes // 2), jnp.float32)
    square = pltpu.VMEM((modes, modes), jnp.float32)
    return pl.pallas_call(
        middle_kernel,
        out_shape=(jax.ShapeDtypeStruct((rows, modes), jnp.float32), part, part),
        in_specs=[SMEM] + [VMEM] * (3 + len(pieces)), out_specs=(VMEM,) * 3,
        scratch_shapes=[pltpu.VMEM((5 * width, rows), jnp.bfloat16), square, square],
        name="middle", compiler_params=pltpu.CompilerParams(vmem_limit_bytes=28 * 2**20), cost_estimate=pl.CostEstimate(flops=20 * rows * modes * modes, bytes_accessed=8 * rows * modes, transcendentals=0),
    )(side, inverse, basis, summed, *pieces)


def last_kernel(inverse, image_ref, out_ref):
    first, second = split(inverse[...], 2)

    def step(rows):
        high, mid = split(image_ref[rows, :], 2)
        out_ref[rows, :] = mul(high, first, (1, 1)) + (mul(mid, first, (1, 1)) + (mul(high, second, (1, 1)) + mul(mid, second, (1, 1))))

    chunks(image_ref.shape[0], step)


def last(inverse, image):
    return pl.pallas_call(
        last_kernel,
        out_shape=jax.ShapeDtypeStruct(image.shape, jnp.float32),
        in_specs=[VMEM] * 2, out_specs=VMEM,
        name="last", compiler_params=pltpu.CompilerParams(vmem_limit_bytes=20 * 2**20), cost_estimate=pl.CostEstimate(flops=8 * image.size * image.shape[1], bytes_accessed=8 * image.size, transcendentals=0),
    )(inverse, image)


BLOCK = 256
ONE = (2, 2, 2, 2)
TWO = (2, 3, 3)


def near_rows(start, dense_ref, high, mid, low, out_ref, held, sems):
    count = out_ref.shape[0] // BLOCK

    def copy(at):
        return pltpu.make_async_copy(dense_ref.at[pl.ds(start + at * BLOCK, BLOCK)], held.at[at], sems.at[at])

    for at in range(count):
        copy(at).start()

    def run(at, carry):
        copy(at).wait()
        top, rest = split(held[at], 2)
        out_ref[pl.ds(pl.multiple_of(at * BLOCK, BLOCK), BLOCK)] = mul(top, high[...]) + (
            mul(top, mid[...]) + (mul(rest, high[...]) + (mul(rest, mid[...]) + mul(top, low[...])))
        )
        return carry

    lax.fori_loop(0, count, run, 0)


def near_first_kernel(dense_ref, field_ref, out_ref, high, mid, low, held, sems):
    def run(at, carry):
        rows = pl.ds(pl.multiple_of(at * BLOCK, BLOCK), BLOCK)
        high[rows, :], mid[rows, :], low[rows, :] = split(field_ref[rows, :], 3)
        return carry

    lax.fori_loop(0, field_ref.shape[0] // BLOCK, run, 0)
    near_rows(0, dense_ref, high, mid, low, out_ref, held, sems)


def near_next_kernel(start, dense_ref, high, mid, low, out_ref, held, sems):
    near_rows(start, dense_ref, high, mid, low, out_ref, held, sems)


def near_of(dense, field, shares):
    rows, depth = dense.shape
    modes = field.shape[1]
    sizes = [rows * share // sum(shares) for share in shares]
    term = jax.ShapeDtypeStruct(field.shape, jnp.bfloat16)
    anywhere = pl.BlockSpec(memory_space=pltpu.HBM)
    pieces, terms, start = [], (), 0
    for at, size in enumerate(sizes):
        out = jax.ShapeDtypeStruct((size, modes), jnp.float32)
        count = size // BLOCK
        settings = dict(
            scratch_shapes=[pltpu.VMEM((count, BLOCK, depth), jnp.float32), pltpu.SemaphoreType.DMA((count,))],
            compiler_params=pltpu.CompilerParams(vmem_limit_bytes=50 * 2**20),
            cost_estimate=pl.CostEstimate(flops=10 * size * depth * modes, bytes_accessed=4 * size * depth, transcendentals=0),
        )
        if at == 0:
            piece, *terms = pl.pallas_call(
                near_first_kernel, out_shape=(out, term, term, term), in_specs=[anywhere, VMEM], out_specs=(VMEM,) * 4,
                name="near_first", **settings,
            )(dense, field)
        else:
            piece = pl.pallas_call(
                functools.partial(near_next_kernel, start), out_shape=out, in_specs=[anywhere, VMEM, VMEM, VMEM],
                out_specs=VMEM, name="near_next", **settings,
            )(dense, *terms)
        pieces.append(piece)
        start += size
    return pieces


def couple_kernel(order, place_ref, masked_ref, *refs):
    blocks, far_ref, near_ref, held = refs[: len(order)], refs[-3], refs[-2], refs[-1]
    tile, group = place_ref[0], place_ref[1]
    width = blocks[0].shape[0] // len(order[0])
    for names, block in zip(order, blocks):
        for at, name in enumerate(names):
            start = pl.multiple_of((tile ^ name) * width, 8)
            held[pl.ds(start, width), :] = block[at * width : (at + 1) * width, :]
    total = jnp.dot(masked_ref[...], held[...], precision=HP, preferred_element_type=jnp.float32)
    held[: total.shape[0], :] = total
    groups = total.shape[0] // width
    count = groups // 2
    for at in range(count):
        near_ref[at * width : (at + 1) * width] = held[pl.ds(pl.multiple_of((group ^ at) * width, 8), width), :]
        far_ref[at * width : (at + 1) * width] = held[pl.ds(pl.multiple_of((group ^ (at + count)) * width, 8), width), :]


def couple(place, masked, blocks, order):
    rows, depth = masked.shape
    modes = blocks[0].shape[1]
    half = jax.ShapeDtypeStruct((rows // 2, modes), jnp.float32)
    return pl.pallas_call(
        functools.partial(couple_kernel, order),
        out_shape=(half, half), in_specs=[SMEM, VMEM] + [VMEM] * len(blocks), out_specs=(VMEM, VMEM),
        scratch_shapes=[pltpu.VMEM((max(rows, depth), modes), jnp.float32)], name="couple", compiler_params=pltpu.CompilerParams(vmem_limit_bytes=8 * 2**20),
        cost_estimate=pl.CostEstimate(flops=12 * rows * depth * modes, bytes_accessed=4 * rows * depth, transcendentals=0),
    )(place, masked, *blocks)


def swap(x, axis, bit):
    return lax.ppermute(x, axis, [(i, i ^ bit) for i in range(lax.axis_size(axis))])


def body(start_block, dense_tiles, basis, coupling, admissible):
    groups = coupling.shape[0]
    width = basis.shape[1]
    span = coupling.shape[3] // width
    tiles = lax.axis_size("tile")
    total_rows = lax.axis_size("grp") * tiles * start_block.shape[0]
    flags = admissible.astype(jnp.float32).reshape(groups, 1, span, 1)
    masked = (coupling.reshape(groups, width, span, width) * flags).reshape(groups * width, span * width)
    dense = dense_tiles[0]
    rows_basis = basis[0]
    group, tile = lax.axis_index("grp"), lax.axis_index("tile")
    place = jnp.stack([tile, group]).astype(jnp.int32)
    side = jnp.stack([group % 2]).astype(jnp.int32)

    def couple_all(coeffs):
        blocks, order, held, names = [coeffs], [(0,)], coeffs, (0,)
        bit = tiles // 2
        while bit:
            got = swap(held, "tile", bit)
            blocks.append(got)
            order.append(tuple(name ^ bit for name in names))
            names = names + order[-1]
            bit //= 2
            if bit:
                held = jnp.concatenate([held, got])
        far, near = couple(place, masked, blocks, tuple(order))
        bit = groups // 2
        while True:
            got = swap(far, "grp", bit)
            near = near + got
            bit //= 2
            if not bit:
                return near
            far, near = near[near.shape[0] // 2 :], near[: near.shape[0] // 2]

    scale = 1.0 / total_rows

    def add_devices(mine, theirs):
        mine = mine + swap(theirs, "grp", 1)
        for axis, bit in sum_rounds(groups, tiles):
            got = swap(mine, axis, bit)
            mine = mine + got
        return mine, swap(mine, "grp", 1)

    summed = couple_all(jnp.dot(rows_basis, start_block, precision=HP))
    image, coeffs, mine, theirs = mix(side, near_of(dense, start_block, ONE), rows_basis, summed)
    mine, theirs = add_devices(mine, theirs)
    summed = couple_all(coeffs)
    image, mine, theirs = middle(side, factor(side, mine, theirs, scale), near_of(dense, image, TWO), rows_basis, summed)
    mine, theirs = add_devices(mine, theirs)
    return last(factor(side, mine, theirs, scale), image)


def sum_rounds(groups, tiles):
    rounds = []
    bit = groups // 2
    while bit > 1:
        rounds.append(("grp", bit))
        bit //= 2
    bit = 1
    while bit < tiles:
        rounds.append(("tile", bit))
        bit *= 2
    return rounds


def solution(mesh):
    placed = (
        P(("grp", "tile"), None),
        P(("grp", "tile"), None, None),
        P(("grp", "tile"), None, None),
        P(None, "tile", None, "grp"),
        P(None, "tile", "grp"),
    )
    return jax.shard_map(body, mesh=mesh, in_specs=placed, out_specs=P(("grp", "tile"), None), check_vma=False)
```

```python
import functools

import jax
import jax.numpy as jnp
from jax import lax
from jax.experimental import pallas as pl
from jax.experimental.pallas import tpu as pltpu
from jax.sharding import PartitionSpec as P


HP = lax.Precision.HIGHEST
SMEM = pl.BlockSpec(memory_space=pltpu.SMEM)
VMEM = pl.BlockSpec(memory_space=pltpu.VMEM)
VREG = (8, 128)


def down(x, row):
    return jnp.broadcast_to(x[row : row + 1, :], VREG)


def factor_inverse(t_ref, out_ref):
    n = t_ref.shape[0]
    halves = range(n // 128)
    lane = lax.broadcasted_iota(jnp.int32, VREG, 1)
    sub = lax.broadcasted_iota(jnp.int32, VREG, 0)
    every = sub < 8
    rows = [t_ref[:8, 128 * g : 128 * g + 128] for g in halves]
    for k in range(0, n, 8):
        h, at = k // 128, k % 128
        cols = [jnp.where(every, jnp.broadcast_to(rows[h][:, at + c : at + c + 1], VREG), 0.0) for c in range(8)]
        inside = (lane >= at) & (lane < at + 8)
        rows[h] = jnp.where(inside, jnp.where(lane - at == sub, 1.0, 0.0), rows[h])
        pivots = jnp.ones(VREG, jnp.float32)
        done = list(rows)
        for j in range(8):
            pivot = down(cols[j], j)
            pivots = jnp.where(sub == j, pivot, pivots)
            f = jnp.where(sub == j, 0.0, cols[j])
            for c in range(j + 1, 8):
                cols[c] = cols[c] - (f * down(cols[c], j)) / pivot
            for g in halves:
                done[g] = jnp.where(sub == j, rows[g], done[g])
                rows[g] = rows[g] - (f * down(rows[g], j)) / pivot
        roots = lax.rsqrt(pivots)
        for g in halves:
            if g > h:
                out = jnp.zeros(VREG, jnp.float32)
            else:
                out = done[g] * roots
                if g == h:
                    out = jnp.where(lane < at + 8, out, 0.0)
            out_ref[k : k + 8, 128 * g : 128 * g + 128] = out
        if k + 8 == n:
            break
        rows = [x / pivots for x in rows]
        wide = [[down(rows[g], i) for i in range(8)] for g in halves]
        for r in range(k + 8, n, 8):
            now = [t_ref[r : r + 8, 128 * g : 128 * g + 128] for g in halves]
            f = [jnp.broadcast_to(now[h][:, at + i : at + i + 1], VREG) for i in range(8)]
            now[h] = jnp.where(inside, 0.0, now[h])
            for g in halves:
                w = wide[g]
                low = (f[0] * w[0] + f[1] * w[1]) + (f[2] * w[2] + f[3] * w[3])
                high = (f[4] * w[4] + f[5] * w[5]) + (f[6] * w[6] + f[7] * w[7])
                now[g] = now[g] - (low + high)
            if r == k + 8:
                rows = now
            else:
                for g in halves:
                    t_ref[r : r + 8, 128 * g : 128 * g + 128] = now[g]


def split(x, parts):
    terms = []
    for at in range(parts):
        terms.append(x.astype(jnp.bfloat16))
        if at + 1 < parts:
            x = x - terms[-1].astype(jnp.float32)
    return terms


def mul(a, b, contract=(1, 0)):
    return lax.dot_general(a, b, (((contract[0],), (contract[1],)), ((), ())), preferred_element_type=jnp.float32)


def triangle_masks(m):
    row = lax.broadcasted_iota(jnp.int32, (m, m), 0)
    col = lax.broadcasted_iota(jnp.int32, (m, m), 1)
    return row, col


def pack_into(side_ref, gram, mine_ref, theirs_ref):
    m = gram.shape[0] // 2
    row, col = triangle_masks(m)
    second = gram[m:, m:]
    cross = gram[m:, :m]
    both = jnp.where(row >= col, gram[:m, :m], second)
    diag = jnp.sum(jnp.where(row == col, second, 0.0), axis=0, keepdims=True)
    south = side_ref[0] == 0
    mine_ref[:m] = jnp.where(south, cross, both)
    theirs_ref[:m] = jnp.where(south, both, cross)
    mine_ref[m:] = jnp.broadcast_to(diag, (8, m))
    theirs_ref[m:] = jnp.broadcast_to(diag, (8, m))


def unpack_into(scale, side_ref, mine_ref, theirs_ref, t_ref):
    m = mine_ref.shape[1]
    row, col = triangle_masks(m)
    south = side_ref[0] == 0
    cross = jnp.where(south, mine_ref[:m], theirs_ref[:m]) * scale
    both = jnp.where(south, theirs_ref[:m], mine_ref[:m]) * scale
    diag = jnp.where(south, theirs_ref[m : m + 1], mine_ref[m : m + 1]) * scale
    flip = both.T
    t_ref[:m, :m] = jnp.where(row >= col, both, flip)
    t_ref[m:, m:] = jnp.where(row == col, jnp.broadcast_to(diag, (m, m)), jnp.where(row < col, both, flip))
    t_ref[m:, :m] = cross
    t_ref[:m, m:] = cross.T


def stack_basis(basis_ref, stacked):
    width = basis_ref.shape[0]
    high, low = split(basis_ref[...], 2)
    for at, part in enumerate((high, low, high, high, low)):
        stacked[at * width : (at + 1) * width] = part


def stack_sums(summed_ref):
    high, mid, low = split(summed_ref[...], 3)
    return jnp.concatenate([high, high, mid, low, mid], axis=0)


def gram_terms(field, total, cross):
    high, mid = split(field, 2)
    total[...] += mul(high, high, (0, 0)) + mul(mid, mid, (0, 0))
    cross[...] += mul(high, mid, (0, 0))


CHUNK = 512


def chunks(rows, step):
    def run(at, carry):
        step(pl.ds(pl.multiple_of(at * CHUNK, CHUNK), CHUNK))
        return carry

    lax.fori_loop(0, rows // CHUNK, run, 0)


def piece_rows(pieces, step):
    start = 0
    for piece in pieces:
        step(pl.ds(start, piece.shape[0]), piece)
        start += piece.shape[0]


def project(two, terms):
    width = two.shape[0] // 2
    high, mid, low = terms
    both = mul(two, high) + mul(two, mid)
    return both[:width] + both[width:] + mul(two[:width], low)


def mix_kernel(side_ref, basis_ref, summed_ref, *refs):
    pieces, outs = refs[:-10], refs[-10:]
    high_ref, mid_ref, low_ref, coeffs_ref, mine_ref, theirs_ref, stacked, total, cross, parts = outs
    width = basis_ref.shape[0]
    stack_basis(basis_ref, stacked)
    sums = stack_sums(summed_ref)
    total[...] = jnp.zeros_like(total)
    cross[...] = jnp.zeros_like(cross)
    parts[...] = jnp.zeros_like(parts)

    def step(rows, piece):
        terms = split(piece[...] + mul(stacked[:, rows], sums, (0, 0)), 3)
        high, mid, _ = terms
        high_ref[rows, :], mid_ref[rows, :], low_ref[rows, :] = terms
        total[...] += mul(high, high, (0, 0)) + mul(mid, mid, (0, 0))
        cross[...] += mul(high, mid, (0, 0))
        parts[...] += project(stacked[: 2 * width, rows], terms)

    piece_rows(pieces, step)
    coeffs_ref[...] = parts[...]
    pack_into(side_ref, total[...] + (cross[...] + cross[...].T), mine_ref, theirs_ref)


def mix(side, pieces, basis, summed):
    rows, modes = basis.shape[1], summed.shape[1]
    width = basis.shape[0]
    part = jax.ShapeDtypeStruct((modes // 2 + 8, modes // 2), jnp.float32)
    square = pltpu.VMEM((modes, modes), jnp.float32)
    term = jax.ShapeDtypeStruct((rows, modes), jnp.bfloat16)
    return pl.pallas_call(
        mix_kernel,
        out_shape=(term, term, term, jax.ShapeDtypeStruct((width, modes), jnp.float32), part, part),
        in_specs=[SMEM, VMEM, VMEM] + [VMEM] * len(pieces), out_specs=(VMEM,) * 6,
        scratch_shapes=[pltpu.VMEM((5 * width, rows), jnp.bfloat16), square, square, pltpu.VMEM((width, modes), jnp.float32)],
        name="mix", compiler_params=pltpu.CompilerParams(vmem_limit_bytes=24 * 2**20), cost_estimate=pl.CostEstimate(flops=12 * rows * modes * modes, bytes_accessed=8 * rows * modes, transcendentals=0),
    )(side, basis, summed, *pieces)


def factor_kernel(scale, side_ref, mine_ref, theirs_ref, out_ref, t_ref):
    unpack_into(scale, side_ref, mine_ref, theirs_ref, t_ref)
    factor_inverse(t_ref, out_ref)


def factor(side, mine, theirs, scale):
    modes = 2 * mine.shape[1]
    return pl.pallas_call(
        functools.partial(factor_kernel, scale),
        out_shape=jax.ShapeDtypeStruct((modes, modes), jnp.float32),
        in_specs=[SMEM, VMEM, VMEM], out_specs=VMEM, scratch_shapes=[pltpu.VMEM((modes, modes), jnp.float32)],
        name="factor", compiler_params=pltpu.CompilerParams(vmem_limit_bytes=16 * 2**20),
        cost_estimate=pl.CostEstimate(flops=40_000_000, bytes_accessed=8 * modes * modes, transcendentals=0),
    )(side, mine, theirs)


def middle_kernel(side_ref, inverse, basis_ref, summed_ref, *refs):
    pieces, (image_ref, out_mine_ref, out_theirs_ref, stacked, total, cross) = refs[:-6], refs[-6:]
    stack_basis(basis_ref, stacked)
    sums = stack_sums(summed_ref)
    total[...] = jnp.zeros_like(total)
    cross[...] = jnp.zeros_like(cross)
    first, second = split(inverse[...], 2)

    def step(rows, piece):
        further = piece[...] + mul(stacked[:, rows], sums, (0, 0))
        high, mid, low = split(further, 3)
        image = (mul(high, first, (1, 1)) + mul(mid, first, (1, 1))) + (mul(high, second, (1, 1)) + (mul(mid, second, (1, 1)) + mul(low, first, (1, 1))))
        image_ref[rows, :] = image
        gram_terms(image, total, cross)

    piece_rows(pieces, step)
    pack_into(side_ref, total[...] + (cross[...] + cross[...].T), out_mine_ref, out_theirs_ref)


def middle(side, inverse, pieces, basis, summed):
    rows, modes = basis.shape[1], summed.shape[1]
    width = basis.shape[0]
    part = jax.ShapeDtypeStruct((modes // 2 + 8, modes // 2), jnp.float32)
    square = pltpu.VMEM((modes, modes), jnp.float32)
    return pl.pallas_call(
        middle_kernel,
        out_shape=(jax.ShapeDtypeStruct((rows, modes), jnp.float32), part, part),
        in_specs=[SMEM] + [VMEM] * (3 + len(pieces)), out_specs=(VMEM,) * 3,
        scratch_shapes=[pltpu.VMEM((5 * width, rows), jnp.bfloat16), square, square],
        name="middle", compiler_params=pltpu.CompilerParams(vmem_limit_bytes=28 * 2**20), cost_estimate=pl.CostEstimate(flops=20 * rows * modes * modes, bytes_accessed=8 * rows * modes, transcendentals=0),
    )(side, inverse, basis, summed, *pieces)


def last_kernel(inverse, image_ref, out_ref):
    first, second = split(inverse[...], 2)

    def step(rows):
        high, mid = split(image_ref[rows, :], 2)
        out_ref[rows, :] = mul(high, first, (1, 1)) + (mul(mid, first, (1, 1)) + (mul(high, second, (1, 1)) + mul(mid, second, (1, 1))))

    chunks(image_ref.shape[0], step)


def last(inverse, image):
    return pl.pallas_call(
        last_kernel,
        out_shape=jax.ShapeDtypeStruct(image.shape, jnp.float32),
        in_specs=[VMEM] * 2, out_specs=VMEM,
        name="last", compiler_params=pltpu.CompilerParams(vmem_limit_bytes=20 * 2**20), cost_estimate=pl.CostEstimate(flops=8 * image.size * image.shape[1], bytes_accessed=8 * image.size, transcendentals=0),
    )(inverse, image)


BLOCK = 256
ONE = (2, 2, 2, 2)
TWO = (2, 3, 3)


def near_kernel(start, dense_ref, high, mid, low, out_ref, held, sems):
    count = out_ref.shape[0] // BLOCK

    def copy(at):
        return pltpu.make_async_copy(dense_ref.at[pl.ds(start + at * BLOCK, BLOCK)], held.at[at], sems.at[at])

    for at in range(count):
        copy(at).start()
    row, col = triangle_masks(BLOCK)

    def run(at, carry):
        copy(at).wait()
        top, rest = split(held[at], 2)
        out = mul(top, high[...]) + (mul(top, mid[...]) + (mul(rest, high[...]) + mul(top, low[...])))
        rows = pl.ds(pl.multiple_of(start + at * BLOCK, BLOCK), BLOCK)
        own = held[at, :, rows]
        own = jnp.where(row == col, own - own.astype(jnp.bfloat16).astype(jnp.float32), 0.0)
        out = out + jnp.sum(own, axis=1, keepdims=True) * mid[rows, :].astype(jnp.float32)
        out_ref[pl.ds(pl.multiple_of(at * BLOCK, BLOCK), BLOCK)] = out
        return carry

    lax.fori_loop(0, count, run, 0)


def near_first_kernel(dense_ref, field_ref, out_ref, high, mid, low, held, sems):
    def run(at, carry):
        rows = pl.ds(pl.multiple_of(at * BLOCK, BLOCK), BLOCK)
        high[rows, :], mid[rows, :], low[rows, :] = split(field_ref[rows, :], 3)
        return carry

    lax.fori_loop(0, field_ref.shape[0] // BLOCK, run, 0)
    near_kernel(0, dense_ref, high, mid, low, out_ref, held, sems)


def near_of(dense, field, terms, shares):
    rows, depth = dense.shape
    modes = (terms[0] if terms else field).shape[1]
    pieces, start = [], 0
    for share in shares:
        size = rows * share // sum(shares)
        count = size // BLOCK
        out = jax.ShapeDtypeStruct((size, modes), jnp.float32)
        settings = dict(
            scratch_shapes=[pltpu.VMEM((count, BLOCK, depth), jnp.float32), pltpu.SemaphoreType.DMA((count,))],
            compiler_params=pltpu.CompilerParams(vmem_limit_bytes=50 * 2**20),
            cost_estimate=pl.CostEstimate(flops=8 * size * depth * modes, bytes_accessed=4 * size * depth, transcendentals=0),
        )
        dense_spec = pl.BlockSpec(memory_space=pltpu.HBM)
        if terms:
            piece = pl.pallas_call(
                functools.partial(near_kernel, start), out_shape=out, in_specs=[dense_spec, VMEM, VMEM, VMEM],
                out_specs=VMEM, name="near", **settings,
            )(dense, *terms)
        else:
            term = jax.ShapeDtypeStruct(field.shape, jnp.bfloat16)
            piece, *terms = pl.pallas_call(
                near_first_kernel, out_shape=(out, term, term, term), in_specs=[dense_spec, VMEM],
                out_specs=(VMEM,) * 4, name="near_first", **settings,
            )(dense, field)
        pieces.append(piece)
        start += size
    return pieces


def couple_kernel(order, place_ref, masked_ref, *refs):
    blocks, far_ref, near_ref, held = refs[: len(order)], refs[-3], refs[-2], refs[-1]
    tile, group = place_ref[0], place_ref[1]
    width = blocks[0].shape[0] // len(order[0])
    for names, block in zip(order, blocks):
        for at, name in enumerate(names):
            start = pl.multiple_of((tile ^ name) * width, 8)
            held[pl.ds(start, width), :] = block[at * width : (at + 1) * width, :]
    total = jnp.dot(masked_ref[...], held[...], precision=HP, preferred_element_type=jnp.float32)
    held[: total.shape[0], :] = total
    groups = total.shape[0] // width
    count = groups // 2
    for at in range(count):
        near_ref[at * width : (at + 1) * width] = held[pl.ds(pl.multiple_of((group ^ at) * width, 8), width), :]
        far_ref[at * width : (at + 1) * width] = held[pl.ds(pl.multiple_of((group ^ (at + count)) * width, 8), width), :]


def couple(place, masked, blocks, order):
    rows, depth = masked.shape
    modes = blocks[0].shape[1]
    half = jax.ShapeDtypeStruct((rows // 2, modes), jnp.float32)
    return pl.pallas_call(
        functools.partial(couple_kernel, order),
        out_shape=(half, half), in_specs=[SMEM, VMEM] + [VMEM] * len(blocks), out_specs=(VMEM, VMEM),
        scratch_shapes=[pltpu.VMEM((max(rows, depth), modes), jnp.float32)], name="couple", compiler_params=pltpu.CompilerParams(vmem_limit_bytes=8 * 2**20),
        cost_estimate=pl.CostEstimate(flops=12 * rows * depth * modes, bytes_accessed=4 * rows * depth, transcendentals=0),
    )(place, masked, *blocks)


def swap(x, axis, bit):
    return lax.ppermute(x, axis, [(i, i ^ bit) for i in range(lax.axis_size(axis))])


def body(start_block, dense_tiles, basis, coupling, admissible):
    groups = coupling.shape[0]
    width = basis.shape[1]
    span = coupling.shape[3] // width
    tiles = lax.axis_size("tile")
    total_rows = lax.axis_size("grp") * tiles * start_block.shape[0]
    flags = admissible.astype(jnp.float32).reshape(groups, 1, span, 1)
    masked = (coupling.reshape(groups, width, span, width) * flags).reshape(groups * width, span * width)
    dense = dense_tiles[0]
    rows_basis = basis[0]
    group, tile = lax.axis_index("grp"), lax.axis_index("tile")
    place = jnp.stack([tile, group]).astype(jnp.int32)
    side = jnp.stack([group % 2]).astype(jnp.int32)

    def couple_all(coeffs):
        blocks, order, held, names = [coeffs], [(0,)], coeffs, (0,)
        bit = tiles // 2
        while bit:
            got = swap(held, "tile", bit)
            blocks.append(got)
            order.append(tuple(name ^ bit for name in names))
            names = names + order[-1]
            bit //= 2
            if bit:
                held = jnp.concatenate([held, got])
        far, near = couple(place, masked, blocks, tuple(order))
        bit = groups // 2
        while True:
            got = swap(far, "grp", bit)
            near = near + got
            bit //= 2
            if not bit:
                return near
            far, near = near[near.shape[0] // 2 :], near[: near.shape[0] // 2]

    scale = 1.0 / total_rows

    def add_devices(mine, theirs):
        mine = mine + swap(theirs, "grp", 1)
        for axis, bit in sum_rounds(groups, tiles):
            got = swap(mine, axis, bit)
            mine = mine + got
        return mine, swap(mine, "grp", 1)

    summed = couple_all(jnp.dot(rows_basis, start_block, precision=HP))
    *terms, coeffs, mine, theirs = mix(side, near_of(dense, start_block, None, ONE), rows_basis, summed)
    mine, theirs = add_devices(mine, theirs)
    summed = couple_all(coeffs)
    image, mine, theirs = middle(side, factor(side, mine, theirs, scale), near_of(dense, None, terms, TWO), rows_basis, summed)
    mine, theirs = add_devices(mine, theirs)
    return last(factor(side, mine, theirs, scale), image)


def sum_rounds(groups, tiles):
    rounds = []
    bit = groups // 2
    while bit > 1:
        rounds.append(("grp", bit))
        bit //= 2
    bit = 1
    while bit < tiles:
        rounds.append(("tile", bit))
        bit *= 2
    return rounds


def solution(mesh):
    placed = (
        P(("grp", "tile"), None),
        P(("grp", "tile"), None, None),
        P(("grp", "tile"), None, None),
        P(None, "tile", None, "grp"),
        P(None, "tile", "grp"),
    )
    return jax.shard_map(body, mesh=mesh, in_specs=placed, out_specs=P(("grp", "tile"), None), check_vma=False)
```
